32 devices in a mesh: grp: 16 (over z, y, x), node: 2 (over core).
Axes of the slice: x: 2, y: 2, z: 4, core: 2. Of those that a mesh axis runs over, the one named last changes fastest.
Arguments:
- grad_out: bfloat16 [6144, 2048], P('grp', 'node'), may hold values from -12 to 12
- gate_prob: float32 [6144], P('grp'), may hold values from 0.05 to 1
- hidden: bfloat16 [6144, 7168], P('grp', 'node'), may hold values from -0.19921875 to 0.19921875
- w_down: bfloat16 [2048, 7168], P(None, 'node'), may hold values from -0.0625 to 0.0625
- slot_counts: int32 [16], P('grp'), may hold values from 0 to 384, as said below
Outputs:
- grad_hidden: bfloat16 [6144, 7168], P('grp', 'node')
- grad_weight: bfloat16 [2048, 7168], P('grp', 'node')
The draws below stay inside these ranges and needn't reach their ends.
Inputs may be any that keep to these rules, and one draw needn't show every extreme that they name: `slot_counts`: each count is a multiple of 128; in every draw some group's count is 384.
All inputs are finite; a program needn't handle non-finite values.
Results may differ from the reference program's by a relative error of at most 0.0057.
Values may be sent and summed in bfloat16 or wider, within the bound.
A program may use at most 128 MiB of HBM per device.

```python
import math
import jax
import jax.numpy as jnp
from jax import lax

D = 2048
FF = 7168
TILE_ROWS = 128
TILES = 3
CAP = 384
GROUPS = 16
ROWS = 6144


def draw_slot_counts(key, part):
    first_key, second_key, third_key = jax.random.split(key, 3)
    choose_full = jax.random.randint(first_key, (GROUPS,), 0, 4)
    light_tiles = jax.random.randint(second_key, (GROUPS,), 0, TILES // 2 + 1)
    tile_counts = jnp.where(choose_full == 0, TILES, light_tiles)
    full_group = jax.random.randint(third_key, (), 0, GROUPS)
    tile_counts = jnp.where(jnp.arange(GROUPS) == full_group, TILES, tile_counts)
    return (tile_counts * TILE_ROWS).astype(jnp.int32)


def raised(entries, rng, source, target, parts, factor):
    owner, partner = [(jnp.arange(entries.shape[position]) // (entries.shape[position] // parts)).reshape([-1 if axis == position else 1 for axis in range(entries.ndim)]) for position in (source, target)]
    chosen = jax.random.permutation(rng, parts)[partner]
    strong = (owner == chosen) | (owner == (partner + parts // 2) % parts)
    return jnp.where(strong, factor * entries, entries)


def shard_levels(own_key, extent, cuts, low, largest):
    def one(position, blocks):
        heights = jax.random.uniform(jax.random.fold_in(jax.random.fold_in(own_key, 6), position), (blocks,), jnp.float32, low / len(cuts), largest / len(cuts))
        return jnp.repeat(jnp.exp(heights), extent[position] // blocks).reshape((-1,) + (1,) * (len(extent) - position - 1))

    loudness = one(*cuts[0])
    for cut in cuts[1:]:
        loudness = loudness * one(*cut)
    return loudness


def gaussian(own_key, extent, width, most, shards=(), kind=jnp.bfloat16):
    values = width * jax.random.normal(own_key, extent, jnp.float32)
    if shards:
        values = values * shard_levels(own_key, extent, shards, -0.22, 0.18)
    return jnp.clip(values, -most, most).astype(kind)


def noise_with(key, shape, spread, limit, cuts, heavy, kind=jnp.bfloat16):
    array = spread * jax.random.normal(key, shape, jnp.float32)
    if cuts:
        array = array * shard_levels(key, shape, cuts, -0.22, 0.18)
    return jnp.clip(raised(array, jax.random.fold_in(key, 3), *heavy), -limit, limit).astype(kind)


def setup_inputs(seed: int = 0) -> dict:
    splits = jax.random.split(jax.random.key(seed), 6)
    return {
        "grad_out": noise_with(splits[0], (ROWS, D), 2.0, 12.0, ((0, 16), (1, 2)), (0, 1, 16, 2.0)),
        "gate_prob": jnp.clip(jnp.exp(math.log(1.0) - 2.9957323 * jax.random.uniform(splits[1], (ROWS,), jnp.float32) ** shard_levels(splits[1], (ROWS,), ((0, 16),), -0.2, 0.2)), 0.05, 1.0),
        "hidden": gaussian(splits[2], (ROWS, FF), 0.03, 0.19921875, ((0, 16), (1, 2))),
        "w_down": gaussian(splits[3], (D, FF), FF ** -0.5, 0.0625, ((1, 2),)),
        "slot_counts": draw_slot_counts(jax.random.fold_in(splits[5], 71), 0),
    }


def reference(grad_out, gate_prob, hidden, w_down, slot_counts):
    scaled = (gate_prob[:, None] * grad_out.astype(jnp.float32)).astype(jnp.bfloat16)
    slot_index = jnp.arange(ROWS, dtype=jnp.int32)
    group_index = (slot_index // CAP).astype(jnp.int32)
    live_slot = (slot_index % CAP) < slot_counts[group_index]
    masked = jnp.where(live_slot[:, None], scaled, jnp.zeros_like(scaled))
    grad_hidden = jnp.dot(masked, w_down, preferred_element_type=jnp.float32)
    grad_hidden = grad_hidden.astype(jnp.bfloat16)
    slot_blocks = masked.reshape(GROUPS, CAP, D)
    hidden_blocks = hidden.reshape(GROUPS, CAP, FF)

    def add_group(running, blocks):
        group_term = jnp.dot(blocks[0].T, blocks[1], preferred_element_type=jnp.float32)
        rounded = lax.optimization_barrier(group_term.astype(jnp.bfloat16))
        return running + rounded.astype(jnp.float32), None

    running, unused = lax.scan(add_group, jnp.zeros((D, FF), jnp.float32), (slot_blocks, hidden_blocks))
    return grad_hidden, running.astype(jnp.bfloat16)
```

```python
import jax
import jax.numpy as jnp
from jax import lax
from jax.sharding import PartitionSpec as P


def body(grad_out, gate_prob, hidden, w_down, slot_counts):
    rows = grad_out.shape[0]
    live = lax.iota(jnp.int32, rows) < slot_counts[0]
    scaled = (gate_prob[:, None] * grad_out.astype(jnp.float32)).astype(jnp.bfloat16)
    scaled = jnp.where(live[:, None], scaled, jnp.zeros_like(scaled))
    gathered = lax.all_gather(scaled, "node", axis=1, tiled=True)
    term = lax.dot_general(
        gathered, hidden, (((0,), (0,)), ((), ())), preferred_element_type=jnp.float32
    ).astype(jnp.bfloat16)
    summed = lax.psum_scatter(term, "grp", scatter_dimension=0, tiled=True)
    grad_hidden = jnp.dot(gathered, w_down, preferred_element_type=jnp.float32).astype(jnp.bfloat16)
    return (grad_hidden, summed)


def solution(mesh):
    return jax.shard_map(
        body,
        mesh=mesh,
        in_specs=(P("grp", "node"), P("grp"), P("grp", "node"), P(None, "node"), P("grp")),
        out_specs=(P("grp", "node"), P("grp", "node")),
        check_vma=False,
    )
```

```python
import functools

import jax
import jax.numpy as jnp
from jax import lax
from jax.experimental import pallas as pl
from jax.experimental.pallas import tpu as pltpu
from jax.sharding import PartitionSpec as P

MESH = pl.DeviceIdType.MESH
LANES = 128
AHEAD = 2
F32, BF16 = jnp.float32, jnp.bfloat16


def added(a, b):
    return (a.astype(F32) + b.astype(F32)).astype(BF16)


def kernel(
    dims, s_ref, st_ref, hid_ref, w_ref, gh_ref, gw_ref,
    g, gt, acc, rx1, rx2, up, dn, wbuf,
    gsend, grecv, send1, recv1, send2, recv2, usend, urecv, dsend, drecv, wsem,
):
    nodes, depth, chunks = dims
    node = lax.axis_index("node")
    me = lax.axis_index("grp")
    mx, my, mz = me % 2, (me // 2) % 2, me // 4
    px, py = 1 - mx, 1 - my
    half = s_ref.shape[1]
    wide = 2 * LANES
    rows = acc.shape[5]
    last = depth - 1
    not_first, not_last = mz > 0, mz < last

    def grp_at(z, y, x):
        return {"grp": (z * 2 + y) * 2 + x}

    to_x, to_y = grp_at(mz, my, px), grp_at(mz, py, mx)
    to_up, to_down = {"grp": me + 4}, {"grp": me - 4}

    barrier = pltpu.get_barrier_semaphore()

    def greet(target):
        pl.semaphore_signal(barrier, inc=1, device_id=target, device_id_type=MESH)

    greet(to_x)
    greet(to_y)
    for off in range(1, nodes):
        greet({"node": (node + off) % nodes})

    @pl.when(not_first)
    def _():
        greet(to_down)

    @pl.when(not_last)
    def _():
        greet(to_up)

    def w_copy(c, slot):
        cols = pl.ds(pl.multiple_of(c * wide, wide), wide)
        return pltpu.make_async_copy(w_ref.at[:, cols], wbuf.at[slot], wsem.at[slot])

    w_copy(0, 0).start()
    pl.semaphore_wait(
        barrier, 1 + nodes + not_first.astype(jnp.int32) + not_last.astype(jnp.int32)
    )

    def remote(src, dst, ssem, rsem, target):
        return pltpu.make_async_remote_copy(
            src_ref=src, dst_ref=dst, send_sem=ssem, recv_sem=rsem,
            device_id=target, device_id_type=MESH,
        )

    def own_rows(i):
        return pl.ds(pl.multiple_of(i * half, half), half)

    def exchange(off):
        target = {"node": (node + off) % nodes}
        return (
            remote(st_ref, gt.at[own_rows(node)], gsend.at[0, off], grecv.at[0, off], target),
            remote(s_ref, g.at[node], gsend.at[1, off], grecv.at[1, off], target),
        )

    for off in range(1, nodes):
        for copy in exchange(off):
            copy.start()
    gt[own_rows(node), :] = st_ref[...]
    g[node] = s_ref[...]
    for off in range(1, nodes):
        for copy in exchange(off):
            copy.wait()

    def first(kind, c):
        if kind == 0:
            src, target = acc.at[0, c, :, :, px], to_x
        else:
            src, target = acc.at[1, c, :, py], to_y
        return remote(src, rx1.at[kind, c], send1.at[kind, c], recv1.at[kind, c], target)

    def second(kind, c):
        if kind == 0:
            src, target = acc.at[0, c, :, py, mx], to_y
        else:
            src, target = acc.at[1, c, :, my, px], to_x
        return remote(src, rx2.at[kind, c], send2.at[kind, c], recv2.at[kind, c], target)

    def line(c, d, rising):
        src = acc.at[:, c, d, my, mx]
        if rising:
            return remote(src, up.at[c, d], usend.at[c, d], urecv.at[c, d], to_up)
        return remote(src, dn.at[c, d], dsend.at[c, d], drecv.at[c, d], to_down)


    def make_term(c):
        cols = pl.ds(pl.multiple_of(c * wide, wide), wide)
        units = hid_ref[:, cols]

        def one(z, carry):
            part = gt[pl.ds(pl.multiple_of(z * 4 * rows, 4 * rows), 4 * rows), :]
            product = jnp.dot(part, units, preferred_element_type=F32).astype(BF16)
            product = product.reshape(2, 2, rows, wide)
            acc[0, c, z] = product[..., :LANES]
            acc[1, c, z] = product[..., LANES:]
            return carry

        lax.fori_loop(0, depth, one, 0)

    def make_hidden(c):
        slot = c % 2
        w_copy(c, slot).wait()

        @pl.when(c + 1 < chunks)
        def _():
            w_copy(c + 1, 1 - slot).start()

        total = jnp.dot(g[0], wbuf[slot, :half, :], preferred_element_type=F32)
        for i in range(1, nodes):
            total += jnp.dot(
                g[i], wbuf[slot, i * half : (i + 1) * half, :], preferred_element_type=F32
            )
        gh_ref[:, pl.ds(pl.multiple_of(c * wide, wide), wide)] = total.astype(BF16)

    def within(c, run):
        @pl.when((c >= 0) & (c < chunks))
        def _():
            run(c)

    def step_make(c):
        make_term(c)
        first(0, c).start()
        first(1, c).start()
        make_hidden(c)

    def step_second(c):
        first(0, c).wait_recv()
        acc[0, c, :, :, mx] = added(acc[0, c, :, :, mx], rx1[0, c])
        second(0, c).start()
        first(1, c).wait_recv()
        acc[1, c, :, my] = added(acc[1, c, :, my], rx1[1, c])
        second(1, c).start()

    def step_column(c):
        for kind in range(2):
            second(kind, c).wait_recv()
            acc[kind, c, :, my, mx] = added(acc[kind, c, :, my, mx], rx2[kind, c])

        @pl.when(mz == 0)
        def _():
            for d in range(last, 0, -1):
                line(c, d, True).start()

        @pl.when(mz == last)
        def _():
            for d in range(last):
                line(c, d, False).start()

    def step_rise(c):
        for d in range(last, 0, -1):
            @pl.when(d >= mz)
            def _():
                line(c, d, True).wait_recv()

            @pl.when(d > mz)
            def _():
                acc[:, c, d, my, mx] = added(acc[:, c, d, my, mx], up[c, d])
                line(c, d, True).start()

    def step_fall(c):
        for d in range(last):
            @pl.when(d <= mz)
            def _():
                line(c, d, False).wait_recv()

            @pl.when(d < mz)
            def _():
                acc[:, c, d, my, mx] = added(acc[:, c, d, my, mx], dn[c, d])
                line(c, d, False).start()

    def step_final(c):
        def put(total):
            for kind in range(2):
                cols = pl.ds(pl.multiple_of(c * wide + kind * LANES, LANES), LANES)
                gw_ref[:, cols] = total[kind].astype(BF16)

        @pl.when(mz == 0)
        def _():
            put(acc[:, c, mz, my, mx].astype(F32) + dn[c, mz].astype(F32))

        @pl.when(mz == last)
        def _():
            put(acc[:, c, mz, my, mx].astype(F32) + up[c, mz].astype(F32))

        @pl.when(not_first & not_last)
        def _():
            put(
                acc[:, c, mz, my, mx].astype(F32)
                + up[c, mz].astype(F32)
                + dn[c, mz].astype(F32)
            )

    def step(t, carry):
        within(t, step_make)
        within(t - AHEAD, step_second)
        column = t - AHEAD - 1
        within(column, step_column)

        @pl.when(not_first)
        def _():
            within(column - mz, step_rise)

        @pl.when(not_last)
        def _():
            within(column - (last - mz), step_fall)

        within(column - last, step_final)
        return carry

    lax.fori_loop(0, chunks + AHEAD + 1 + last, step, 0)

    def drain(c, carry):
        for kind in range(2):
            first(kind, c).wait_send()
            second(kind, c).wait_send()
        for d in range(depth):
            @pl.when(d > mz)
            def _():
                line(c, d, True).wait_send()

            @pl.when(d < mz)
            def _():
                line(c, d, False).wait_send()
        return carry

    lax.fori_loop(0, chunks, drain, 0)


def body(grad_out, gate_prob, hidden, w_down, slot_counts):
    slots, half = grad_out.shape
    nodes, groups = lax.axis_size("node"), lax.axis_size("grp")
    depth = groups // 4
    model = w_down.shape[0]
    rows = model // groups
    units = hidden.shape[1]
    wide = 2 * LANES
    chunks = -(-units // wide)
    extra = chunks * wide - units
    live = lax.iota(jnp.int32, slots) < slot_counts[0]
    scaled = (gate_prob[:, None] * grad_out.astype(F32)).astype(BF16)
    scaled = jnp.where(live[:, None], scaled, jnp.zeros_like(scaled))
    if extra:
        hidden = jnp.pad(hidden, ((0, 0), (0, extra)))
        w_down = jnp.pad(w_down, ((0, 0), (0, extra)))
    dma = pltpu.SemaphoreType.DMA
    vmem = pl.BlockSpec(memory_space=pltpu.VMEM)
    grad_hidden, grad_weight = pl.pallas_call(
        functools.partial(kernel, (nodes, depth, chunks)),
        out_shape=(
            jax.ShapeDtypeStruct((slots, chunks * wide), BF16),
            jax.ShapeDtypeStruct((rows, chunks * wide), BF16),
        ),
        in_specs=[vmem, vmem, vmem, pl.BlockSpec(memory_space=pl.ANY)],
        out_specs=(vmem, vmem),
        scratch_shapes=[
            pltpu.VMEM((nodes, slots, half), BF16),
            pltpu.VMEM((model, slots), BF16),
            pltpu.VMEM((2, chunks, depth, 2, 2, rows, LANES), BF16),
            pltpu.VMEM((2, chunks, depth, 2, rows, LANES), BF16),
            pltpu.VMEM((2, chunks, depth, rows, LANES), BF16),
            pltpu.VMEM((chunks, depth, 2, rows, LANES), BF16),
            pltpu.VMEM((chunks, depth, 2, rows, LANES), BF16),
            pltpu.VMEM((2, model, wide), BF16),
            dma((2, nodes)),
            dma((2, nodes)),
            dma((2, chunks)),
            dma((2, chunks)),
            dma((2, chunks)),
            dma((2, chunks)),
            dma((chunks, depth)),
            dma((chunks, depth)),
            dma((chunks, depth)),
            dma((chunks, depth)),
            dma((2,)),
        ],
        compiler_params=pltpu.CompilerParams(
            collective_id=0, has_side_effects=True, vmem_limit_bytes=60 * 1024 * 1024
        ),
    )(scaled, scaled.T, hidden, w_down)
    return grad_hidden[:, :units], grad_weight[:, :units]


def solution(mesh):
    return jax.shard_map(
        body,
        mesh=mesh,
        in_specs=(P("grp", "node"), P("grp"), P("grp", "node"), P(None, "node"), P("grp")),
        out_specs=(P("grp", "node"), P("grp", "node")),
        check_vma=False,
    )
```

```python
import functools

import jax
import jax.numpy as jnp
from jax import lax
from jax.experimental import pallas as pl
from jax.experimental.pallas import tpu as pltpu
from jax.sharding import PartitionSpec as P

MESH = pl.DeviceIdType.MESH
LANES = 128
AHEAD = 2
HOP = 1
F32, BF16 = jnp.float32, jnp.bfloat16


def added(a, b):
    return (a.astype(F32) + b.astype(F32)).astype(BF16)


def kernel(
    dims, s_ref, st_ref, hid_any, w_ref, gh_ref, gw_ref,
    g, gt, acc, rx1, rx2, up, dn, wbuf, hid_ref, zacc, zup, zdn, za, zb,
    gsend, grecv, send1, recv1, send2, recv2, usend, urecv, dsend, drecv, wsem,
    zusend, zurecv, zdsend, zdrecv, zsend1, zrecv1, zsend2, zrecv2, hsem,
):
    nodes, depth, chunks, zchunks = dims
    total_chunks = chunks + zchunks
    node = lax.axis_index("node")
    me = lax.axis_index("grp")
    mx, my, mz = me % 2, (me // 2) % 2, me // 4
    px, py = 1 - mx, 1 - my
    half = s_ref.shape[1]
    wide = 2 * LANES
    rows = acc.shape[5]
    last = depth - 1
    not_first, not_last = mz > 0, mz < last

    def grp_at(z, y, x):
        return {"grp": (z * 2 + y) * 2 + x}

    to_x, to_y = grp_at(mz, my, px), grp_at(mz, py, mx)
    to_up, to_down = {"grp": me + 4}, {"grp": me - 4}

    barrier = pltpu.get_barrier_semaphore()

    def greet(target):
        pl.semaphore_signal(barrier, inc=1, device_id=target, device_id_type=MESH)

    greet(to_x)
    greet(to_y)
    for off in range(1, nodes):
        greet({"node": (node + off) % nodes})

    @pl.when(not_first)
    def _():
        greet(to_down)

    @pl.when(not_last)
    def _():
        greet(to_up)

    def w_copy(c, slot):
        cols = pl.ds(pl.multiple_of(c * wide, wide), wide)
        return pltpu.make_async_copy(w_ref.at[:, cols], wbuf.at[slot], wsem.at[slot])

    fetch = pltpu.make_async_copy(hid_any, hid_ref, hsem)
    fetch.start()
    w_copy(0, 0).start()
    pl.semaphore_wait(
        barrier, 1 + nodes + not_first.astype(jnp.int32) + not_last.astype(jnp.int32)
    )

    def remote(src, dst, ssem, rsem, target):
        return pltpu.make_async_remote_copy(
            src_ref=src, dst_ref=dst, send_sem=ssem, recv_sem=rsem,
            device_id=target, device_id_type=MESH,
        )

    def own_rows(i):
        return pl.ds(pl.multiple_of(i * half, half), half)

    def exchange(off):
        target = {"node": (node + off) % nodes}
        return (
            remote(st_ref, gt.at[own_rows(node)], gsend.at[0, off], grecv.at[0, off], target),
            remote(s_ref, g.at[node], gsend.at[1, off], grecv.at[1, off], target),
        )

    for off in range(1, nodes):
        for copy in exchange(off):
            copy.start()
    gt[own_rows(node), :] = st_ref[...]
    g[node] = s_ref[...]
    for off in range(1, nodes):
        for copy in exchange(off):
            copy.wait()
    fetch.wait()

    def first(kind, c):
        if kind == 0:
            src, target = acc.at[0, c, :, :, px], to_x
        else:
            src, target = acc.at[1, c, :, py], to_y
        return remote(src, rx1.at[kind, c], send1.at[kind, c], recv1.at[kind, c], target)

    def second(kind, c):
        if kind == 0:
            src, target = acc.at[0, c, :, py, mx], to_y
        else:
            src, target = acc.at[1, c, :, my, px], to_x
        return remote(src, rx2.at[kind, c], send2.at[kind, c], recv2.at[kind, c], target)

    def line(c, d, rising):
        src = acc.at[:, c, d, my, mx]
        if rising:
            return remote(src, up.at[c, d], usend.at[c, d], urecv.at[c, d], to_up)
        return remote(src, dn.at[c, d], dsend.at[c, d], drecv.at[c, d], to_down)


    def make_term(into, c, column):
        cols = pl.ds(pl.multiple_of(column * wide, wide), wide)
        units = hid_ref[:, cols]

        def one(z, carry):
            part = gt[pl.ds(pl.multiple_of(z * 4 * rows, 4 * rows), 4 * rows), :]
            product = jnp.dot(part, units, preferred_element_type=F32).astype(BF16)
            product = product.reshape(2, 2, rows, wide)
            into[0, c, z] = product[..., :LANES]
            into[1, c, z] = product[..., LANES:]
            return carry

        lax.fori_loop(0, depth, one, 0)

    def make_hidden(c):
        slot = c % 2
        w_copy(c, slot).wait()

        @pl.when(c + 1 < total_chunks)
        def _():
            w_copy(c + 1, 1 - slot).start()

        total = jnp.dot(g[0], wbuf[slot, :half, :], preferred_element_type=F32)
        for i in range(1, nodes):
            total += jnp.dot(
                g[i], wbuf[slot, i * half : (i + 1) * half, :], preferred_element_type=F32
            )
        gh_ref[:, pl.ds(pl.multiple_of(c * wide, wide), wide)] = total.astype(BF16)

    def within(c, run, count=chunks):
        @pl.when((c >= 0) & (c < count))
        def _():
            run(c)

    def step_make(c):
        make_term(acc, c, c)
        first(0, c).start()
        first(1, c).start()

    def step_second(c):
        first(0, c).wait_recv()
        acc[0, c, :, :, mx] = added(acc[0, c, :, :, mx], rx1[0, c])
        second(0, c).start()
        first(1, c).wait_recv()
        acc[1, c, :, my] = added(acc[1, c, :, my], rx1[1, c])
        second(1, c).start()

    def step_column(c):
        for kind in range(2):
            second(kind, c).wait_recv()
            acc[kind, c, :, my, mx] = added(acc[kind, c, :, my, mx], rx2[kind, c])

        @pl.when(mz == 0)
        def _():
            for d in range(last, 0, -1):
                line(c, d, True).start()

        @pl.when(mz == last)
        def _():
            for d in range(last):
                line(c, d, False).start()

    def step_rise(c):
        for d in range(last, 0, -1):
            @pl.when(d >= mz)
            def _():
                line(c, d, True).wait_recv()

            @pl.when(d > mz)
            def _():
                acc[:, c, d, my, mx] = added(acc[:, c, d, my, mx], up[c, d])
                line(c, d, True).start()

    def step_fall(c):
        for d in range(last):
            @pl.when(d <= mz)
            def _():
                line(c, d, False).wait_recv()

            @pl.when(d < mz)
            def _():
                acc[:, c, d, my, mx] = added(acc[:, c, d, my, mx], dn[c, d])
                line(c, d, False).start()

    def step_final(c):
        def put(total):
            for kind in range(2):
                cols = pl.ds(pl.multiple_of(c * wide + kind * LANES, LANES), LANES)
                gw_ref[:, cols] = total[kind].astype(BF16)

        @pl.when(mz == 0)
        def _():
            put(acc[:, c, mz, my, mx].astype(F32) + dn[c, mz].astype(F32))

        @pl.when(mz == last)
        def _():
            put(acc[:, c, mz, my, mx].astype(F32) + up[c, mz].astype(F32))

        @pl.when(not_first & not_last)
        def _():
            put(
                acc[:, c, mz, my, mx].astype(F32)
                + up[c, mz].astype(F32)
                + dn[c, mz].astype(F32)
            )

    def zline(q, d, rising):
        src = zacc.at[:, q, d]
        if rising:
            return remote(src, zup.at[q, d], zusend.at[q, d], zurecv.at[q, d], to_up)
        return remote(src, zdn.at[q, d], zdsend.at[q, d], zdrecv.at[q, d], to_down)

    def zfirst(kind, q):
        if kind == 0:
            src, target = zacc.at[0, q, mz, :, px], to_x
        else:
            src, target = zacc.at[1, q, mz, py], to_y
        return remote(src, za.at[kind, q], zsend1.at[kind, q], zrecv1.at[kind, q], target)

    def zsecond(kind, q):
        if kind == 0:
            src, target = zacc.at[0, q, mz, py, mx], to_y
        else:
            src, target = zacc.at[1, q, mz, my, px], to_x
        return remote(src, zb.at[kind, q], zsend2.at[kind, q], zrecv2.at[kind, q], target)

    def zmake(t):
        @pl.when(t % last == 0)
        def _():
            make_term(zacc, t // last, chunks + t // last)

    def zrise(m):
        q, d = m // last, last - m % last

        @pl.when(not_first & (d >= mz))
        def _():
            zline(q, d, True).wait_recv()
            zacc[:, q, d] = added(zacc[:, q, d], zup[q, d])

        @pl.when(d > mz)
        def _():
            zline(q, d, True).start()

    def zfall(m):
        q, d = m // last, m % last

        @pl.when(not_last & (d <= mz))
        def _():
            zline(q, d, False).wait_recv()
            zacc[:, q, d] = added(zacc[:, q, d], zdn[q, d])

        @pl.when(d < mz)
        def _():
            zline(q, d, False).start()

    def every_last(m, run):
        @pl.when((m >= 0) & (m % last == 0) & (m < zchunks * last))
        def _():
            run(m // last)

    def zstep_first(q):
        zfirst(0, q).start()
        zfirst(1, q).start()

    def zstep_second(q):
        zfirst(0, q).wait_recv()
        zacc[0, q, mz, :, mx] = added(zacc[0, q, mz, :, mx], za[0, q])
        zsecond(0, q).start()
        zfirst(1, q).wait_recv()
        zacc[1, q, mz, my] = added(zacc[1, q, mz, my], za[1, q])
        zsecond(1, q).start()

    def zstep_final(q):
        for kind in range(2):
            zsecond(kind, q).wait_recv()
            cols = pl.ds(
                pl.multiple_of((chunks + q) * wide + kind * LANES, LANES), LANES
            )
            gw_ref[:, cols] = added(zacc[kind, q, mz, my, mx], zb[kind, q])

    def step(t, carry):
        within(t, step_make)
        within(t, zmake, zchunks * last)
        @pl.when(mz == 0)
        def _():
            within(t, zrise, zchunks * last)

        @pl.when(mz == last)
        def _():
            within(t, zfall, zchunks * last)

        within(t, make_hidden, total_chunks)
        within(t - AHEAD, step_second)

        @pl.when(not_first)
        def _():
            within(t - HOP * mz, zrise, zchunks * last)

        @pl.when(not_last)
        def _():
            within(t - HOP * (last - mz), zfall, zchunks * last)

        done = t - HOP * last
        every_last(done, zstep_first)
        every_last(done - 1, zstep_second)
        every_last(done - 2, zstep_final)
        column = t - AHEAD - 1
        within(column, step_column)

        @pl.when(not_first)
        def _():
            within(column - HOP * mz, step_rise)

        @pl.when(not_last)
        def _():
            within(column - HOP * (last - mz), step_fall)

        within(column - HOP * last, step_final)
        return carry

    steps = max(chunks + AHEAD + 1 + HOP * last, (zchunks - 1 + HOP) * last + 3, total_chunks)
    lax.fori_loop(0, steps, step, 0)

    def drain(c, carry):
        for kind in range(2):
            first(kind, c).wait_send()
            second(kind, c).wait_send()
        for d in range(depth):
            @pl.when(d > mz)
            def _():
                line(c, d, True).wait_send()

            @pl.when(d < mz)
            def _():
                line(c, d, False).wait_send()
        return carry

    lax.fori_loop(0, chunks, drain, 0)

    def zdrain(q, carry):
        for kind in range(2):
            zfirst(kind, q).wait_send()
            zsecond(kind, q).wait_send()
        for d in range(depth):
            @pl.when(d > mz)
            def _():
                zline(q, d, True).wait_send()

            @pl.when(d < mz)
            def _():
                zline(q, d, False).wait_send()
        return carry

    lax.fori_loop(0, zchunks, zdrain, 0)


def body(grad_out, gate_prob, hidden, w_down, slot_counts):
    slots, half = grad_out.shape
    nodes, groups = lax.axis_size("node"), lax.axis_size("grp")
    depth = groups // 4
    model = w_down.shape[0]
    rows = model // groups
    units = hidden.shape[1]
    wide = 2 * LANES
    total_chunks = -(-units // wide)
    zchunks = max(1, round(total_chunks * 3 / 14))
    chunks = total_chunks - zchunks
    extra = total_chunks * wide - units
    live = lax.iota(jnp.int32, slots) < slot_counts[0]
    scaled = (gate_prob[:, None] * grad_out.astype(F32)).astype(BF16)
    scaled = jnp.where(live[:, None], scaled, jnp.zeros_like(scaled))
    if extra:
        hidden = jnp.pad(hidden, ((0, 0), (0, extra)))
        w_down = jnp.pad(w_down, ((0, 0), (0, extra)))
    dma = pltpu.SemaphoreType.DMA
    vmem = pl.BlockSpec(memory_space=pltpu.VMEM)
    grad_hidden, grad_weight = pl.pallas_call(
        functools.partial(kernel, (nodes, depth, chunks, zchunks)),
        out_shape=(
            jax.ShapeDtypeStruct((slots, total_chunks * wide), BF16),
            jax.ShapeDtypeStruct((rows, total_chunks * wide), BF16),
        ),
        in_specs=[vmem, vmem] + [pl.BlockSpec(memory_space=pl.ANY)] * 2,
        out_specs=(vmem, vmem),
        scratch_shapes=[
            pltpu.VMEM((nodes, slots, half), BF16),
            pltpu.VMEM((model, slots), BF16),
            pltpu.VMEM((2, chunks, depth, 2, 2, rows, LANES), BF16),
            pltpu.VMEM((2, chunks, depth, 2, rows, LANES), BF16),
            pltpu.VMEM((2, chunks, depth, rows, LANES), BF16),
            pltpu.VMEM((chunks, depth, 2, rows, LANES), BF16),
            pltpu.VMEM((chunks, depth, 2, rows, LANES), BF16),
            pltpu.VMEM((2, model, wide), BF16),
            pltpu.VMEM((slots, total_chunks * wide), BF16),
            pltpu.VMEM((2, zchunks, depth, 2, 2, rows, LANES), BF16),
            pltpu.VMEM((zchunks, depth, 2, 2, 2, rows, LANES), BF16),
            pltpu.VMEM((zchunks, depth, 2, 2, 2, rows, LANES), BF16),
            pltpu.VMEM((2, zchunks, 2, rows, LANES), BF16),
            pltpu.VMEM((2, zchunks, rows, LANES), BF16),
            dma((2, nodes)),
            dma((2, nodes)),
            dma((2, chunks)),
            dma((2, chunks)),
            dma((2, chunks)),
            dma((2, chunks)),
            dma((chunks, depth)),
            dma((chunks, depth)),
            dma((chunks, depth)),
            dma((chunks, depth)),
            dma((2,)),
            dma((zchunks, depth)),
            dma((zchunks, depth)),
            dma((zchunks, depth)),
            dma((zchunks, depth)),
            dma((2, zchunks)),
            dma((2, zchunks)),
            dma((2, zchunks)),
            dma((2, zchunks)),
            dma(()),
        ],
        compiler_params=pltpu.CompilerParams(
            collective_id=0, has_side_effects=True, vmem_limit_bytes=60 * 1024 * 1024
        ),
    )(scaled, scaled.T, hidden, w_down)
    return grad_hidden[:, :units], grad_weight[:, :units]


def solution(mesh):
    return jax.shard_map(
        body,
        mesh=mesh,
        in_specs=(P("grp", "node"), P("grp"), P("grp", "node"), P(None, "node"), P("grp")),
        out_specs=(P("grp", "node"), P("grp", "node")),
        check_vma=False,
    )
```

```python
import functools

import jax
import jax.numpy as jnp
from jax import lax
from jax.experimental import pallas as pl
from jax.experimental.pallas import tpu as pltpu
from jax.sharding import PartitionSpec as P

MESH = pl.DeviceIdType.MESH
LANES = 128
AHEAD = 1
HOP = 2
F32, BF16 = jnp.float32, jnp.bfloat16


def added(a, b):
    return (a.astype(F32) + b.astype(F32)).astype(BF16)


def kernel(
    dims, s_ref, hid_any, w_ref, gh_ref, gw_ref,
    g, acc, rx1, rx2, up, dn, wbuf, hid_ref, zacc, zup, zdn, za, zb,
    gsend, grecv, send1, recv1, send2, recv2, usend, urecv, dsend, drecv, wsem,
    zusend, zurecv, zdsend, zdrecv, zsend1, zrecv1, zsend2, zrecv2, hsem,
):
    nodes, depth, chunks, zchunks = dims
    total_chunks = chunks + zchunks
    node = lax.axis_index("node")
    me = lax.axis_index("grp")
    mx, my, mz = me % 2, (me // 2) % 2, me // 4
    px, py = 1 - mx, 1 - my
    half = s_ref.shape[1]
    wide = 2 * LANES
    rows = acc.shape[5]
    last = depth - 1
    not_first, not_last = mz > 0, mz < last

    def grp_at(z, y, x):
        return {"grp": (z * 2 + y) * 2 + x}

    to_x, to_y = grp_at(mz, my, px), grp_at(mz, py, mx)
    to_up, to_down = {"grp": me + 4}, {"grp": me - 4}

    barrier = pltpu.get_barrier_semaphore()

    def greet(target):
        pl.semaphore_signal(barrier, inc=1, device_id=target, device_id_type=MESH)

    greet(to_x)
    greet(to_y)
    for off in range(1, nodes):
        greet({"node": (node + off) % nodes})

    @pl.when(not_first)
    def _():
        greet(to_down)

    @pl.when(not_last)
    def _():
        greet(to_up)

    def w_copy(c, slot):
        cols = pl.ds(pl.multiple_of(c * wide, wide), wide)
        return pltpu.make_async_copy(w_ref.at[:, cols], wbuf.at[slot], wsem.at[slot])

    fetch = pltpu.make_async_copy(hid_any, hid_ref, hsem)
    fetch.start()
    w_copy(0, 0).start()
    pl.semaphore_wait(
        barrier, 1 + nodes + not_first.astype(jnp.int32) + not_last.astype(jnp.int32)
    )

    def remote(src, dst, ssem, rsem, target):
        return pltpu.make_async_remote_copy(
            src_ref=src, dst_ref=dst, send_sem=ssem, recv_sem=rsem,
            device_id=target, device_id_type=MESH,
        )

    def exchange(off):
        target = {"node": (node + off) % nodes}
        return remote(s_ref, g.at[node], gsend.at[off], grecv.at[off], target)

    for off in range(1, nodes):
        exchange(off).start()
    g[node] = s_ref[...]
    for off in range(1, nodes):
        exchange(off).wait()
    fetch.wait()

    def first(kind, c):
        if kind == 0:
            src, target = acc.at[0, c, :, :, px], to_x
        else:
            src, target = acc.at[1, c, :, py], to_y
        return remote(src, rx1.at[kind, c], send1.at[kind, c], recv1.at[kind, c], target)

    def second(kind, c):
        if kind == 0:
            src, target = acc.at[0, c, :, py, mx], to_y
        else:
            src, target = acc.at[1, c, :, my, px], to_x
        return remote(src, rx2.at[kind, c], send2.at[kind, c], recv2.at[kind, c], target)

    def line(c, d, rising):
        src = acc.at[:, c, d, my, mx]
        if rising:
            return remote(src, up.at[c, d], usend.at[c, d], urecv.at[c, d], to_up)
        return remote(src, dn.at[c, d], dsend.at[c, d], drecv.at[c, d], to_down)


    def make_term(into, c, column):
        cols = pl.ds(pl.multiple_of(column * wide, wide), wide)
        units = hid_ref[:, cols]

        def one(z, carry):
            tall = 4 * rows
            start = pl.multiple_of((z * tall) % half, tall)
            part = g[(z * tall) // half, :, pl.ds(start, tall)]
            product = lax.dot_general(
                part, units, (((0,), (0,)), ((), ())), preferred_element_type=F32
            ).astype(BF16)
            product = product.reshape(2, 2, rows, wide)
            into[0, c, z] = product[..., :LANES]
            into[1, c, z] = product[..., LANES:]
            return carry

        lax.fori_loop(0, depth, one, 0)

    def make_hidden(c):
        slot = c % 2
        w_copy(c, slot).wait()

        @pl.when(c + 1 < total_chunks)
        def _():
            w_copy(c + 1, 1 - slot).start()

        total = jnp.dot(g[0], wbuf[slot, :half, :], preferred_element_type=F32)
        for i in range(1, nodes):
            total += jnp.dot(
                g[i], wbuf[slot, i * half : (i + 1) * half, :], preferred_element_type=F32
            )
        gh_ref[:, pl.ds(pl.multiple_of(c * wide, wide), wide)] = total.astype(BF16)

    def within(c, run, count=chunks):
        @pl.when((c >= 0) & (c < count))
        def _():
            run(c)

    def step_make(c):
        make_term(acc, c, c)
        first(0, c).start()
        first(1, c).start()

    def step_second(c):
        first(0, c).wait_recv()
        acc[0, c, :, :, mx] = added(acc[0, c, :, :, mx], rx1[0, c])
        second(0, c).start()
        first(1, c).wait_recv()
        acc[1, c, :, my] = added(acc[1, c, :, my], rx1[1, c])
        second(1, c).start()

    def step_column(c):
        for kind in range(2):
            second(kind, c).wait_recv()
            acc[kind, c, :, my, mx] = added(acc[kind, c, :, my, mx], rx2[kind, c])

        @pl.when(mz == 0)
        def _():
            for d in range(last, 0, -1):
                line(c, d, True).start()

        @pl.when(mz == last)
        def _():
            for d in range(last):
                line(c, d, False).start()

    def step_rise(c):
        for d in range(last, 0, -1):
            @pl.when(d >= mz)
            def _():
                line(c, d, True).wait_recv()

            @pl.when(d > mz)
            def _():
                acc[:, c, d, my, mx] = added(acc[:, c, d, my, mx], up[c, d])
                line(c, d, True).start()

    def step_fall(c):
        for d in range(last):
            @pl.when(d <= mz)
            def _():
                line(c, d, False).wait_recv()

            @pl.when(d < mz)
            def _():
                acc[:, c, d, my, mx] = added(acc[:, c, d, my, mx], dn[c, d])
                line(c, d, False).start()

    def step_final(c):
        def put(total):
            for kind in range(2):
                cols = pl.ds(pl.multiple_of(c * wide + kind * LANES, LANES), LANES)
                gw_ref[:, cols] = total[kind].astype(BF16)

        @pl.when(mz == 0)
        def _():
            put(acc[:, c, mz, my, mx].astype(F32) + dn[c, mz].astype(F32))

        @pl.when(mz == last)
        def _():
            put(acc[:, c, mz, my, mx].astype(F32) + up[c, mz].astype(F32))

        @pl.when(not_first & not_last)
        def _():
            put(
                acc[:, c, mz, my, mx].astype(F32)
                + up[c, mz].astype(F32)
                + dn[c, mz].astype(F32)
            )

    def zline(q, d, rising):
        src = zacc.at[:, q, d]
        if rising:
            return remote(src, zup.at[q, d], zusend.at[q, d], zurecv.at[q, d], to_up)
        return remote(src, zdn.at[q, d], zdsend.at[q, d], zdrecv.at[q, d], to_down)

    def zfirst(kind, q):
        if kind == 0:
            src, target = zacc.at[0, q, mz, :, px], to_x
        else:
            src, target = zacc.at[1, q, mz, py], to_y
        return remote(src, za.at[kind, q], zsend1.at[kind, q], zrecv1.at[kind, q], target)

    def zsecond(kind, q):
        if kind == 0:
            src, target = zacc.at[0, q, mz, py, mx], to_y
        else:
            src, target = zacc.at[1, q, mz, my, px], to_x
        return remote(src, zb.at[kind, q], zsend2.at[kind, q], zrecv2.at[kind, q], target)

    def zmake(t):
        @pl.when(t % last == 0)
        def _():
            make_term(zacc, t // last, chunks + t // last)

    def zrise(m):
        q, d = m // last, last - m % last

        @pl.when(not_first & (d >= mz))
        def _():
            zline(q, d, True).wait_recv()
            zacc[:, q, d] = added(zacc[:, q, d], zup[q, d])

        @pl.when(d > mz)
        def _():
            zline(q, d, True).start()

    def zfall(m):
        q, d = m // last, m % last

        @pl.when(not_last & (d <= mz))
        def _():
            zline(q, d, False).wait_recv()
            zacc[:, q, d] = added(zacc[:, q, d], zdn[q, d])

        @pl.when(d < mz)
        def _():
            zline(q, d, False).start()

    def every_last(m, run):
        @pl.when((m >= 0) & (m % last == 0) & (m < zchunks * last))
        def _():
            run(m // last)

    def zstep_first(q):
        zfirst(0, q).start()
        zfirst(1, q).start()

    def zstep_second(q):
        zfirst(0, q).wait_recv()
        zacc[0, q, mz, :, mx] = added(zacc[0, q, mz, :, mx], za[0, q])
        zsecond(0, q).start()
        zfirst(1, q).wait_recv()
        zacc[1, q, mz, my] = added(zacc[1, q, mz, my], za[1, q])
        zsecond(1, q).start()

    def zstep_final(q):
        for kind in range(2):
            zsecond(kind, q).wait_recv()
            cols = pl.ds(
                pl.multiple_of((chunks + q) * wide + kind * LANES, LANES), LANES
            )
            gw_ref[:, cols] = added(zacc[kind, q, mz, my, mx], zb[kind, q])

    def step(t, carry):
        within(t, step_make)
        within(t, zmake, zchunks * last)
        @pl.when(mz == 0)
        def _():
            within(t, zrise, zchunks * last)

        @pl.when(mz == last)
        def _():
            within(t, zfall, zchunks * last)

        within(t, make_hidden, total_chunks)
        within(t - AHEAD, step_second)

        @pl.when(not_first)
        def _():
            within(t - HOP * mz, zrise, zchunks * last)

        @pl.when(not_last)
        def _():
            within(t - HOP * (last - mz), zfall, zchunks * last)

        done = t - HOP * last
        every_last(done, zstep_first)
        every_last(done - 1, zstep_second)
        every_last(done - 2, zstep_final)
        column = t - AHEAD - 1
        within(column, step_column)

        @pl.when(not_first)
        def _():
            within(column - HOP * mz, step_rise)

        @pl.when(not_last)
        def _():
            within(column - HOP * (last - mz), step_fall)

        within(column - HOP * last, step_final)
        return carry

    steps = max(chunks + AHEAD + 1 + HOP * last, (zchunks - 1 + HOP) * last + 3, total_chunks)
    lax.fori_loop(0, steps, step, 0)

    def drain(c, carry):
        for kind in range(2):
            first(kind, c).wait_send()
            second(kind, c).wait_send()
        for d in range(depth):
            @pl.when(d > mz)
            def _():
                line(c, d, True).wait_send()

            @pl.when(d < mz)
            def _():
                line(c, d, False).wait_send()
        return carry

    lax.fori_loop(0, chunks, drain, 0)

    def zdrain(q, carry):
        for kind in range(2):
            zfirst(kind, q).wait_send()
            zsecond(kind, q).wait_send()
        for d in range(depth):
            @pl.when(d > mz)
            def _():
                zline(q, d, True).wait_send()

            @pl.when(d < mz)
            def _():
                zline(q, d, False).wait_send()
        return carry

    lax.fori_loop(0, zchunks, zdrain, 0)


def body(grad_out, gate_prob, hidden, w_down, slot_counts):
    slots, half = grad_out.shape
    nodes, groups = lax.axis_size("node"), lax.axis_size("grp")
    depth = groups // 4
    model = w_down.shape[0]
    rows = model // groups
    units = hidden.shape[1]
    wide = 2 * LANES
    total_chunks = -(-units // wide)
    zchunks = max(1, round(total_chunks * 3 / 14))
    chunks = total_chunks - zchunks
    extra = total_chunks * wide - units
    live = lax.iota(jnp.int32, slots) < slot_counts[0]
    scaled = (gate_prob[:, None] * grad_out.astype(F32)).astype(BF16)
    scaled = jnp.where(live[:, None], scaled, jnp.zeros_like(scaled))
    if extra:
        hidden = jnp.pad(hidden, ((0, 0), (0, extra)))
        w_down = jnp.pad(w_down, ((0, 0), (0, extra)))
    dma = pltpu.SemaphoreType.DMA
    vmem = pl.BlockSpec(memory_space=pltpu.VMEM)
    grad_hidden, grad_weight = pl.pallas_call(
        functools.partial(kernel, (nodes, depth, chunks, zchunks)),
        out_shape=(
            pltpu.VMEM((slots, total_chunks * wide), BF16),
            pltpu.VMEM((rows, total_chunks * wide), BF16),
        ),
        in_specs=[vmem] + [pl.BlockSpec(memory_space=pl.ANY)] * 2,
        out_specs=(vmem, vmem),
        scratch_shapes=[
            pltpu.VMEM((nodes, slots, half), BF16),
            pltpu.VMEM((2, chunks, depth, 2, 2, rows, LANES), BF16),
            pltpu.VMEM((2, chunks, depth, 2, rows, LANES), BF16),
            pltpu.VMEM((2, chunks, depth, rows, LANES), BF16),
            pltpu.VMEM((chunks, depth, 2, rows, LANES), BF16),
            pltpu.VMEM((chunks, depth, 2, rows, LANES), BF16),
            pltpu.VMEM((2, model, wide), BF16),
            pltpu.VMEM((slots, total_chunks * wide), BF16),
            pltpu.VMEM((2, zchunks, depth, 2, 2, rows, LANES), BF16),
            pltpu.VMEM((zchunks, depth, 2, 2, 2, rows, LANES), BF16),
            pltpu.VMEM((zchunks, depth, 2, 2, 2, rows, LANES), BF16),
            pltpu.VMEM((2, zchunks, 2, rows, LANES), BF16),
            pltpu.VMEM((2, zchunks, rows, LANES), BF16),
            dma((nodes,)),
            dma((nodes,)),
            dma((2, chunks)),
            dma((2, chunks)),
            dma((2, chunks)),
            dma((2, chunks)),
            dma((chunks, depth)),
            dma((chunks, depth)),
            dma((chunks, depth)),
            dma((chunks, depth)),
            dma((2,)),
            dma((zchunks, depth)),
            dma((zchunks, depth)),
            dma((zchunks, depth)),
            dma((zchunks, depth)),
            dma((2, zchunks)),
            dma((2, zchunks)),
            dma((2, zchunks)),
            dma((2, zchunks)),
            dma(()),
        ],
        compiler_params=pltpu.CompilerParams(
            collective_id=0, has_side_effects=True, vmem_limit_bytes=54 * 1024 * 1024
        ),
    )(scaled, hidden, w_down)
    return grad_hidden[:, :units], grad_weight[:, :units]


def solution(mesh):
    return jax.shard_map(
        body,
        mesh=mesh,
        in_specs=(P("grp", "node"), P("grp"), P("grp", "node"), P(None, "node"), P("grp")),
        out_specs=(P("grp", "node"), P("grp", "node")),
        check_vma=False,
    )
```
